512 devices in a mesh: section: 8 (over x, core), tensor: 2 (over y_hi), expert: 32 (over z, y_lo).
Axes of the slice: x: 4, y: 8 (y_hi: 2, y_lo: 4; y = y_hi * 4 + y_lo), z: 8, core: 2. Of those that a mesh axis runs over, the one named last changes fastest.
Arguments:
- saved_inputs: bfloat16 [8, 2, 2048, 2048], P('section', None, 'expert', 'tensor'), may hold values from -64 to 64
- cot_in: bfloat16 [8, 2048, 2048], P('section', 'expert', 'tensor'), may hold values from -6 to 6
- loss_grad: bfloat16 [2048, 2048], P('expert', 'tensor'), may hold values from -6 to 6
- expert_ids: int32 [8, 2, 2048, 4], P('section', None, 'expert'), may hold values from 0 to 15, all different within a row; in each aligned block of 64 rows (0 to 63, 64 to 127, ..., all dimensions but the last counted through in order) at most 24 rows name the same one
- route_weights: float32 [8, 2, 2048, 4], P('section', None, 'expert'), may hold values from 0.05 to 0.5
- norm_gain: float32 [8, 2048], P('section', 'tensor'), may hold values from 0.12 to 8
- w_gate: bfloat16 [8, 32, 2048, 384], P('section', 'expert', 'tensor'), may hold values from -0.125 to 0.125
- w_up: bfloat16 [8, 32, 2048, 384], P('section', 'expert', 'tensor'), may hold values from -0.125 to 0.125
- w_down: bfloat16 [8, 32, 384, 2048], P('section', 'expert', None, 'tensor'), may hold values from -0.21875 to 0.21875
Outputs:
- input_grads: bfloat16 [8, 2, 2048, 2048], P('section', None, 'expert', 'tensor')
The draws below stay inside these ranges and needn't reach their ends.
Inputs may be any that keep to these rules, and one draw needn't show every extreme that they name: `expert_ids`: each row names 4 different experts. Within each aligned block of 64 rows (the rows of one device in one micro-batch of one layer) no expert is named by more than 24 rows, and in some blocks one expert is named by exactly 24.
All inputs are finite; a program needn't handle non-finite values.
Results may differ from the reference program's by a relative error of at most 0.028.
Values may be sent and summed in bfloat16 or wider, within the bound.
No kernel may reach another device: no remote copies, remote signals or barrier semaphores. Data moves between devices by JAX's collectives and lax.ppermute only.
A program may use at most 64 MiB of HBM per device.

```python
import math
import jax
import jax.numpy as jnp
import numpy as np
from jax import lax

D = 2048
FF = 768
TOK_MB = 64
LAYERS = 8
EXPERTS = 16
TOP = 4
CAP = 24
TOKENS = 2048
N_TENSOR = 2
N_EXPERT = 32


def draw_saved_inputs(key, part):
    key_base, key_cols, key_rows = jax.random.split(key, 3)
    ramp = 3.0 ** (jnp.arange(D, dtype=jnp.float32) / D)
    columns = ramp * 10.0 ** (0.5 * jax.random.uniform(key_cols, (D,), jnp.float32))
    row_scale = 10.0 ** (jax.random.uniform(key_rows, (LAYERS, 2, TOKENS, 1), jnp.float32) - 0.5)
    base = jnp.clip(jax.random.normal(key_base, (LAYERS, 2, TOKENS, D), jnp.float32), -6.0, 6.0)
    return (base * columns * row_scale / 3.0).astype(jnp.bfloat16)


def draw_norm_gain(key, part):
    key_rough = jax.random.fold_in(key, 17)
    place = jnp.arange(D, dtype=jnp.float32) / D
    ramp = 0.25 * 16.0 ** place
    rough = 10.0 ** (0.3 * jax.random.uniform(key_rough, (LAYERS, D), jnp.float32) - 0.15)
    return (ramp[None, :] * rough).astype(jnp.float32)


def block_scale(stream_key, dims, cuts, smallest, top_value):
    def one(dim, blocks):
        steps = jax.random.uniform(jax.random.fold_in(jax.random.fold_in(stream_key, 6), dim), (blocks,), jnp.float32, smallest / len(cuts), top_value / len(cuts))
        return jnp.repeat(jnp.exp(steps), dims[dim] // blocks).reshape((-1,) + (1,) * (len(dims) - dim - 1))

    loudness = one(*cuts[0])
    for cut in cuts[1:]:
        loudness = loudness * one(*cut)
    return loudness


def routed_block(key, own, number, rows, count, top, reach, lean):
    sequence = jax.random.permutation(key, count)
    packed, usual = shares(count, rows * top, reach, lean, True), shares(count, rows * top, reach, lean, False)
    places = jnp.arange(count)

    def named(tallies, rotation):
        used = int((tallies > 0).sum())
        fixed = max(1, used // 4)
        shifted = fixed + (places - fixed + rotation * (used - fixed)) % max(1, count - fixed)
        return jnp.zeros((count,), jnp.int32).at[sequence[jnp.where(places < fixed, places, shifted)]].set(jnp.asarray(tallies, jnp.int32))

    tallies = jnp.where(number % 4 == 0, named(packed, number // 4), named(usual, number - number // 4 - 1))
    mixed = jax.random.permutation(jax.random.fold_in(own, 3), count)
    donor, taker = mixed[0:count // 2 * 2:2], mixed[1:count // 2 * 2:2]
    slack = jnp.minimum(tallies[donor] - 1, reach - tallies[taker]) // 2
    slack = jnp.where((donor == sequence[0]) | (taker == sequence[0]) | (tallies[taker] == 0), 0, jnp.maximum(slack, 0))
    shifted = jax.random.randint(jax.random.fold_in(own, 4), (count // 2,), 0, 1 << 20) % (slack + 1)
    tallies = tallies.at[donor].add(-shifted).at[taker].add(shifted)
    members = jnp.searchsorted(jnp.cumsum(tallies), jnp.arange(rows * top), side="right").astype(jnp.int32)
    listing = members.reshape(top, rows).T
    listing = listing[jax.random.permutation(jax.random.fold_in(own, 1), rows)]
    rotation = jax.random.randint(jax.random.fold_in(own, 2), (rows, 1), 0, top)
    return jnp.take_along_axis(listing, (jnp.arange(top)[None, :] + rotation) % top, axis=1)


def shares(amount, total, bound, lean, full):
    loads = [(1 << 20) // math.isqrt(grade ** lean) + 1 for grade in range(1, amount + 1)]
    largest = bound if full else min(bound, max(-(-total // amount), total * loads[0] // sum(loads)))
    least = 1 if total - largest >= amount - 1 else 0
    holding, rest = [largest] + [least] * (amount - 1), total - largest - least * (amount - 1)
    while rest > 0:
        movable = [i for i in range(1, amount) if holding[i] < largest] or [i for i in range(1, amount) if holding[i] < bound]
        whole, remaining = sum([loads[i] for i in movable]), rest
        for i in movable:
            more = min(bound - holding[i], max(1, remaining * loads[i] // whole), rest)
            holding[i] = holding[i] + more
            rest = rest - more
    return np.array(holding)


def bell_draw(stream_key, shape, width, bound, cuts=(), kind=jnp.bfloat16):
    drawn = jax.random.normal(stream_key, shape, jnp.float32) * width
    if len(cuts) > 0:
        drawn = block_scale(stream_key, shape, cuts, -0.22, 0.18) * drawn
    return jnp.clip(drawn, min=-bound, max=bound).astype(kind)


def setup_inputs(seed: int = 0) -> dict:
    key_of = jax.random.split(jax.random.key(seed), 10)
    saved_inputs = draw_saved_inputs(jax.random.fold_in(key_of[9], 71), 0)
    cot_in = bell_draw(key_of[1], (LAYERS, TOKENS, D), 1.0, 6.0, ((0, 8), (1, 32), (2, 2)))
    loss_grad = bell_draw(key_of[2], (TOKENS, D), 1.0, 6.0, ((0, 32), (1, 2)))
    expert_ids_keys = jax.random.split(jax.random.fold_in(key_of[3], 1), LAYERS * 2 * TOKENS // TOK_MB)
    expert_ids_turns = jax.random.permutation(jax.random.fold_in(key_of[3], 3), LAYERS * 2 * TOKENS // TOK_MB)
    expert_ids = jax.vmap(lambda own, number: routed_block(jax.random.fold_in(key_of[3], 2), own, number, TOK_MB, EXPERTS, TOP, CAP, 2))(expert_ids_keys, expert_ids_turns).reshape((LAYERS, 2, TOKENS, TOP))
    route_weights = jnp.clip(jnp.exp(math.log(0.5) - 2.3025851 * jax.random.uniform(key_of[4], (LAYERS, 2, TOKENS, TOP), jnp.float32) ** block_scale(key_of[4], (LAYERS, 2, TOKENS, TOP), ((0, 8), (2, 32)), -0.2, 0.2)), 0.05, 0.5)
    norm_gain = draw_norm_gain(jax.random.fold_in(key_of[9], 71), 0)
    w_gate = bell_draw(key_of[6], (LAYERS, 2 * EXPERTS, D, FF // 2), D ** -0.5, 0.125, ((0, 8), (1, 32), (2, 2)))
    w_up = bell_draw(key_of[7], (LAYERS, 2 * EXPERTS, D, FF // 2), D ** -0.5, 0.125, ((0, 8), (1, 32), (2, 2)))
    w_down = bell_draw(key_of[8], (LAYERS, 2 * EXPERTS, FF // 2, D), FF ** -0.5, 0.21875, ((0, 8), (1, 32), (3, 2)))
    return {"saved_inputs": saved_inputs, "cot_in": cot_in, "loss_grad": loss_grad, "expert_ids": expert_ids, "route_weights": route_weights, "norm_gain": norm_gain, "w_gate": w_gate, "w_up": w_up, "w_down": w_down}


epsilon = 1e-06

def silu_grad(values):
    sigma = jax.nn.sigmoid(values)
    return sigma * (1.0 + values * (1.0 - sigma))

def product(left, right):
    return jnp.dot(left.astype(jnp.float32), right.astype(jnp.float32), precision=lax.Precision.HIGHEST)

def rounded(values):
    return lax.optimization_barrier(values.astype(jnp.bfloat16)).astype(jnp.float32)

def slot_tables(route_ids, weights):
    blocks = route_ids.reshape(N_EXPERT, TOK_MB * TOP)
    onehot = (blocks[:, :, None] == jnp.arange(EXPERTS, dtype=jnp.int32)[None, None, :]).astype(jnp.int32)
    before = jnp.cumsum(onehot, axis=1) - onehot
    position = lax.optimization_barrier(jnp.sum(before * onehot, axis=2))
    source = jnp.arange(N_EXPERT, dtype=jnp.int32)[:, None]
    flat_slot = (blocks * (N_EXPERT * CAP) + source * CAP + position).reshape(-1).astype(jnp.int32)
    token_index = jnp.repeat(jnp.arange(TOKENS, dtype=jnp.int32), TOP)
    slot_total = EXPERTS * N_EXPERT * CAP
    token_of = jnp.full((slot_total,), TOKENS, jnp.int32).at[flat_slot].set(token_index)
    weight_of = jnp.zeros((slot_total,), jnp.float32).at[flat_slot].set(weights.reshape(-1))
    return (token_of, weight_of)

def expert_back(operands):
    rows_in, rows_grad, gate_weights, up_weights, down_weights = operands
    group = D // N_TENSOR
    pieces = []
    for part_index in range(2):
        gate_sum = jnp.zeros((rows_in.shape[0], FF // 2), jnp.float32)
        up_sum = jnp.zeros((rows_in.shape[0], FF // 2), jnp.float32)
        hidden = jnp.zeros((rows_in.shape[0], FF // 2), jnp.float32)
        for rank_index in range(N_TENSOR):
            low = rank_index * group
            high = low + group
            gate_sum = gate_sum + rounded(product(rows_in[:, low:high], gate_weights[part_index, low:high]))
            up_sum = up_sum + rounded(product(rows_in[:, low:high], up_weights[part_index, low:high]))
            hidden = hidden + rounded(product(rows_grad[:, low:high], down_weights[part_index][:, low:high].T))
        grad_gate = (hidden * up_sum * silu_grad(gate_sum)).astype(jnp.bfloat16)
        grad_up = (hidden * jax.nn.silu(gate_sum)).astype(jnp.bfloat16)
        grad_piece = product(grad_gate, gate_weights[part_index].T) + product(grad_up, up_weights[part_index].T)
        pieces.append(grad_piece.astype(jnp.bfloat16))
    return jnp.stack(pieces)

def layer_back(inputs, incoming, route_ids, weights, gain_row, gate_weights, up_weights, down_weights):
    values = inputs.astype(jnp.float32)
    squares = lax.optimization_barrier(jnp.sum(values * values, axis=1, keepdims=True))
    root_mean = jnp.sqrt(squares / D + epsilon)
    normed = values / root_mean
    expert_input = (normed * gain_row[None, :]).astype(jnp.bfloat16)
    token_of, weight_of = slot_tables(route_ids, weights)
    padded_input = jnp.concatenate([expert_input, jnp.zeros((1, D), jnp.bfloat16)], axis=0)
    padded_grad = jnp.concatenate([incoming, jnp.zeros((1, D), jnp.bfloat16)], axis=0)
    rows_in = padded_input[token_of].reshape(EXPERTS, N_EXPERT * CAP, D)
    rows_grad = (weight_of[:, None] * padded_grad[token_of].astype(jnp.float32)).astype(jnp.bfloat16)
    rows_grad = rows_grad.reshape(EXPERTS, N_EXPERT * CAP, D)
    pieces = lax.map(expert_back, (rows_in, rows_grad, gate_weights.reshape(EXPERTS, 2, D, FF // 2), up_weights.reshape(EXPERTS, 2, D, FF // 2), down_weights.reshape(EXPERTS, 2, FF // 2, D)))
    summed = lax.optimization_barrier(jnp.sum(pieces.astype(jnp.float32), axis=1)).reshape(-1, D)
    cot_normed = jax.ops.segment_sum(summed, token_of, TOKENS + 1)[:TOKENS]
    scaled = gain_row[None, :] * cot_normed
    inner = lax.optimization_barrier(jnp.sum(normed * scaled, axis=1, keepdims=True))
    return (incoming.astype(jnp.float32) + (scaled - normed * (inner / D)) / root_mean).astype(jnp.bfloat16)

def reference(saved_inputs, cot_in, loss_grad, expert_ids, route_weights, norm_gain, w_gate, w_up, w_down):

    def first_layer(layer):
        return layer_back(saved_inputs[layer, 0], cot_in[layer], expert_ids[layer, 0], route_weights[layer, 0], norm_gain[layer], w_gate[layer], w_up[layer], w_down[layer])
    first_pass = lax.map(first_layer, jnp.arange(LAYERS, dtype=jnp.int32))
    following = jnp.concatenate([first_pass[1:], loss_grad[None]], axis=0)

    def second_layer(layer):
        return layer_back(saved_inputs[layer, 1], following[layer], expert_ids[layer, 1], route_weights[layer, 1], norm_gain[layer], w_gate[layer], w_up[layer], w_down[layer])
    second_pass = lax.map(second_layer, jnp.arange(LAYERS, dtype=jnp.int32))
    return jnp.stack([first_pass, second_pass], axis=1)
```

```python
import jax
import jax.numpy as jnp
from jax import lax
from jax.experimental import pallas as pl
from jax.experimental.pallas import tpu as pltpu
from jax.sharding import PartitionSpec as P

D = 2048
epsilon = 1e-06
VMEM_LIMIT = 48 * 1024 * 1024


def whole(count):
    return [pl.BlockSpec(memory_space=pltpu.VMEM) for _ in range(count)]


def call(kernel, out_shape, *operands, scalar=None):
    specs = whole(len(operands))
    if scalar is not None:
        specs = [pl.BlockSpec(memory_space=pltpu.SMEM)] + specs
        operands = (scalar, *operands)
    out_specs = (
        whole(len(out_shape))
        if isinstance(out_shape, (list, tuple))
        else pl.BlockSpec(memory_space=pltpu.VMEM)
    )
    return pl.pallas_call(
        kernel,
        out_shape=out_shape,
        in_specs=specs,
        out_specs=out_specs,
        compiler_params=pltpu.CompilerParams(vmem_limit_bytes=VMEM_LIMIT),
    )(*operands)


def dot(left, right):
    return jnp.dot(left, right, preferred_element_type=jnp.float32)


def dot_last(left, right):
    return lax.dot_general(
        left, right, (((1,), (1,)), ((), ())), preferred_element_type=jnp.float32
    )


def dot_first(left, right):
    return lax.dot_general(
        left, right, (((0,), (0,)), ((), ())), preferred_element_type=jnp.float32
    )


def swap(array):
    return lax.ppermute(array, "tensor", [(0, 1), (1, 0)])


def exchange(array):
    return lax.all_to_all(array, ("tensor", "expert"), split_axis=0, concat_axis=0, tiled=True)


def pack_kernel(rows_ref, pick_a, pick_b, scale_a, scale_b, out_ref):
    peers, eight, lanes = out_ref.shape
    width = rows_ref.shape[1]
    half = width // 2
    rows = rows_ref[...]
    first = dot(pick_a[...], rows) * scale_a[...]
    stacked = jnp.concatenate([rows[:, :half], rows[:, half:]], axis=0)
    second = dot(pick_b[...], stacked) * scale_b[...]
    out_ref[:, :, :width] = first.astype(jnp.bfloat16).reshape(peers, eight, width)
    out_ref[:, :, width:] = second.astype(jnp.bfloat16).reshape(peers, eight, half)


def pack_plain_kernel(rows_ref, pick_a, pick_b, out_ref):
    peers, eight, lanes = out_ref.shape
    width = rows_ref.shape[1]
    half = width // 2
    rows = rows_ref[...]
    stacked = jnp.concatenate([rows[:, :half], rows[:, half:]], axis=0)
    out_ref[:, :, :width] = (
        dot(pick_a[...], rows).astype(jnp.bfloat16).reshape(peers, eight, width)
    )
    out_ref[:, :, width:] = (
        dot(pick_b[...], stacked).astype(jnp.bfloat16).reshape(peers, eight, half)
    )


def expert_kernel(
    rank_ref, rows_ref, grads_ref, gate_0, up_0, down_0, gate_1, up_1, down_1, out_ref
):
    peers, eight, lanes = out_ref.shape
    width = 2 * lanes // 3
    half = width // 2
    sources = peers // 2
    count = sources * eight
    rank = rank_ref[0]
    starts = (rank * sources, (1 - rank) * sources)
    gates, ups, downs = (gate_0, gate_1), (up_0, up_1), (down_0, down_1)
    low = lax.broadcasted_iota(jnp.int32, (sources, eight, half), 1) < eight // 2

    def unpack(ref, start):
        part = ref[pl.ds(start, sources), :, :]
        tail = part[:, :, width:]
        zero = jnp.zeros_like(tail)
        tail = jnp.concatenate([jnp.where(low, tail, zero), jnp.where(low, zero, tail)], axis=2)
        return jnp.concatenate(
            [part[:, :, :width].reshape(count, width), tail.reshape(count, width)], axis=0
        )

    def joined(values):
        tail = values[count:].reshape(sources, eight, values.shape[1])
        tail = tail + pltpu.roll(tail, eight // 2, 1)
        return jnp.concatenate([values[:count], tail.reshape(count, values.shape[1])], axis=0)

    gate = up = hidden = 0.0
    for i in range(2):
        part = unpack(rows_ref, starts[i])
        gate = gate + dot(part, gates[i][...])
        up = up + dot(part, ups[i][...])
        hidden = hidden + dot_last(unpack(grads_ref, starts[i]), downs[i][...])
    gate, up, hidden = joined(gate), joined(up), joined(hidden)
    sigma = jax.nn.sigmoid(gate)
    grad_gate = (hidden * up * (sigma * (1.0 + gate * (1.0 - sigma)))).astype(jnp.bfloat16)
    grad_up = (hidden * (gate * sigma)).astype(jnp.bfloat16)
    for i in range(2):
        piece = dot_last(grad_gate, gates[i][...]) + dot_last(grad_up, ups[i][...])
        tail = piece[count:].reshape(sources, eight, width)
        tail = jnp.where(low, tail[:, :, :half], tail[:, :, half:])
        out_ref[pl.ds(starts[i], sources), :, :width] = (
            piece[:count].astype(jnp.bfloat16).reshape(sources, eight, width)
        )
        out_ref[pl.ds(starts[i], sources), :, width:] = tail.astype(jnp.bfloat16)


def combine_kernel(pieces_ref, pick_a, pick_b, normed_ref, gain_ref, scaled_ref, inner_ref):
    peers, eight, lanes = pieces_ref.shape
    tokens, width = scaled_ref.shape
    half = width // 2
    pieces = pieces_ref[...].reshape(peers * eight, lanes)
    first = dot_first(pick_a[...], pieces[:, :width])
    second = dot_first(pick_b[...], pieces[:, width:])
    second = jnp.concatenate([second[:tokens], second[tokens:]], axis=1)
    scaled = gain_ref[...] * (first + second)
    scaled_ref[...] = scaled
    inner_ref[...] = jnp.sum(normed_ref[...] * scaled, axis=1, keepdims=True) + jnp.zeros(
        inner_ref.shape, jnp.float32
    )


def tables(ids, weights, peers, experts, share):
    tokens = ids.shape[0]
    named = ids[:, :, None] == jnp.arange(experts, dtype=jnp.int32)[None, None, :]
    member = jnp.sum(named.astype(jnp.float32), axis=1)
    weight_of = jnp.sum(jnp.where(named, weights[:, :, None], 0.0), axis=1)
    earlier = (
        jnp.arange(tokens, dtype=jnp.int32)[:, None] > jnp.arange(tokens, dtype=jnp.int32)[None, :]
    )
    before = dot(earlier.astype(jnp.bfloat16), member.astype(jnp.bfloat16))
    place = jnp.where(member > 0.0, before, -1.0).T.astype(jnp.int32)
    place = place[None, :, None, None, :]
    ranks = jnp.arange(2, dtype=jnp.int32)[:, None, None, None, None]
    rows = jnp.arange(8, dtype=jnp.int32)[None, None, None, :, None]
    shape = (2, experts, 2, 8, tokens)
    hit_a = jnp.broadcast_to(place == ranks * share + rows, shape)
    hit_b = jnp.broadcast_to(place == ranks * share + 8 + rows % 4, shape)
    weight_t = weight_of.T[None, :, None, None, :]
    scale_a = jnp.sum(jnp.where(hit_a, weight_t, 0.0), axis=4).reshape(peers * 8, 1)
    scale_b = jnp.sum(jnp.where(hit_b, weight_t, 0.0), axis=4).reshape(peers * 8, 1)
    hit_b = jnp.concatenate([hit_b & (rows < 4), hit_b & (rows >= 4)], axis=4)
    pick_a = hit_a.reshape(peers * 8, tokens).astype(jnp.bfloat16)
    pick_b = hit_b.reshape(peers * 8, 2 * tokens).astype(jnp.bfloat16)
    return pick_a, pick_b, scale_a, scale_b


def local(
    saved_inputs, cot_in, loss_grad, expert_ids, route_weights, norm_gain, w_gate, w_up, w_down
):
    section_count = lax.axis_size("section")
    at_last = lax.axis_index("section") == section_count - 1
    rank = lax.axis_index("tensor").astype(jnp.int32)[None]
    peers = 2 * lax.axis_size("expert")
    experts = lax.axis_size("expert") // 2
    tokens, width = saved_inputs.shape[2:]
    per_token = expert_ids.shape[3]
    capacity = 3 * tokens * per_token // (2 * experts)
    share = capacity // 2
    gain_row = norm_gain[0][None, :]
    own = (w_gate[0, 0], w_up[0, 0], w_down[0, 0])
    message = jax.ShapeDtypeStruct((peers, 8, share * width // 8), jnp.bfloat16)

    picks = [tables(expert_ids[0, m], route_weights[0, m], peers, experts, share) for m in (0, 1)]

    def send_grads(micro, incoming):
        return exchange(call(pack_kernel, message, incoming, *picks[micro]))

    grads_0 = send_grads(0, cot_in[0])
    inputs = saved_inputs[0].astype(jnp.float32)
    squares = jnp.sum(inputs * inputs, axis=2)
    squares = squares + swap(squares)
    root_mean = jnp.sqrt(squares / D + epsilon)[:, :, None]
    normed = inputs / root_mean
    expert_input = (normed * gain_row).astype(jnp.bfloat16)
    rows = [
        exchange(call(pack_plain_kernel, message, expert_input[m], *picks[m][:2])) for m in (0, 1)
    ]
    other = [swap(w) for w in own]

    def layer_step(micro, incoming, grads):
        pieces = exchange(
            call(expert_kernel, message, rows[micro], grads, *own, *other, scalar=rank)
        )
        scaled, inner = call(
            combine_kernel,
            [
                jax.ShapeDtypeStruct((tokens, width), jnp.float32),
                jax.ShapeDtypeStruct((tokens, 128), jnp.float32),
            ],
            pieces,
            *picks[micro][:2],
            normed[micro],
            gain_row,
        )
        inner = inner[:, 0]
        inner = inner + swap(inner)
        result = (
            incoming.astype(jnp.float32)
            + (scaled - normed[micro] * (inner / D)[:, None]) / root_mean[micro]
        )
        return result.astype(jnp.bfloat16)

    first_grads = layer_step(0, cot_in[0], grads_0)
    pairs = [(i, i - 1) for i in range(1, section_count)]
    passed = lax.ppermute(first_grads, "section", pairs)
    incoming = jnp.where(at_last, loss_grad, passed)
    second_grads = layer_step(1, incoming, send_grads(1, incoming))
    return jnp.stack([first_grads, second_grads])[None]


def solution(mesh):
    in_specs = (
        P("section", None, "expert", "tensor"),
        P("section", "expert", "tensor"),
        P("expert", "tensor"),
        P("section", None, "expert", None),
        P("section", None, "expert", None),
        P("section", "tensor"),
        P("section", "expert", "tensor", None),
        P("section", "expert", "tensor", None),
        P("section", "expert", None, "tensor"),
    )
    out_specs = P("section", None, "expert", "tensor")
    return jax.shard_map(local, mesh=mesh, in_specs=in_specs, out_specs=out_specs, check_vma=False)
```

```python
import jax
import jax.numpy as jnp
from jax import lax
from jax.experimental import pallas as pl
from jax.experimental.pallas import tpu as pltpu
from jax.sharding import PartitionSpec as P

D = 2048
epsilon = 1e-06
VMEM_LIMIT = 48 * 1024 * 1024
EXTRA = 128
CAPACITY = 24


def call(kernel, out_shape, *operands):
    def spec():
        return pl.BlockSpec(memory_space=pltpu.VMEM)

    several = isinstance(out_shape, (list, tuple))
    return pl.pallas_call(
        kernel,
        out_shape=out_shape,
        in_specs=[spec() for _ in operands],
        out_specs=[spec() for _ in out_shape] if several else spec(),
        compiler_params=pltpu.CompilerParams(vmem_limit_bytes=VMEM_LIMIT),
    )(*operands)


def dot(left, right):
    return jnp.dot(left, right, preferred_element_type=jnp.float32)


def dot_last(left, right):
    return lax.dot_general(
        left, right, (((1,), (1,)), ((), ())), preferred_element_type=jnp.float32
    )


def dot_first(left, right):
    return lax.dot_general(
        left, right, (((0,), (0,)), ((), ())), preferred_element_type=jnp.float32
    )


def swap(array):
    return lax.ppermute(array, "tensor", [(0, 1), (1, 0)])


def pair_swap(array):
    pairs = [(i, i ^ 1) for i in range(lax.axis_size("expert"))]
    return lax.ppermute(array, "expert", pairs)


def exchange(array):
    count = lax.axis_size("expert")
    groups = [list(range(parity, count, 2)) for parity in range(2)]
    return lax.all_to_all(
        array, "expert", split_axis=0, concat_axis=0, tiled=True, axis_index_groups=groups
    )


def tables_kernel(ids_ref, weights_ref, pick_ref, scale_ref):
    micros, per_token, tokens = ids_ref.shape
    slots = pick_ref.shape[1]
    experts = slots // CAPACITY
    capacity = CAPACITY
    row = lax.broadcasted_iota(jnp.int32, (tokens, tokens), 0)
    col = lax.broadcasted_iota(jnp.int32, (tokens, tokens), 1)
    earlier = (row < col).astype(jnp.bfloat16)
    expert = lax.broadcasted_iota(jnp.int32, (experts, tokens), 0)
    slot = lax.broadcasted_iota(jnp.int32, (capacity, tokens), 0).astype(jnp.float32)
    for m in range(micros):
        member = jnp.zeros((experts, tokens), jnp.float32)
        weight = jnp.zeros((experts, tokens), jnp.float32)
        for k in range(per_token):
            hit = ids_ref[m, k : k + 1, :] == expert
            member = jnp.where(hit, 1.0, member)
            weight = jnp.where(hit, weights_ref[m, k : k + 1, :], weight)
        before = dot(member.astype(jnp.bfloat16), earlier)
        place = jnp.where(member > 0.0, before, -1.0)
        for e in range(experts):
            hit = slot == place[e : e + 1, :]
            pick_ref[m, e * capacity : (e + 1) * capacity, :] = jnp.where(hit, 1.0, 0.0).astype(
                jnp.bfloat16
            )
            scale_ref[m, e * capacity : (e + 1) * capacity, :] = jnp.sum(
                jnp.where(hit, weight[e : e + 1, :], 0.0), axis=1, keepdims=True
            )


def normalized(inputs, root):
    return inputs.astype(jnp.float32) / root


def pack_kernel(inputs_ref, grads_ref, gain_ref, root_ref, pick_ref, scale_ref, both_ref, next_ref):
    experts, twice, width = both_ref.shape
    capacity = twice // 2
    gain = gain_ref[...]
    for m, out_ref in ((0, both_ref), (1, next_ref)):
        rows = (normalized(inputs_ref[m], root_ref[m]) * gain).astype(jnp.bfloat16)
        sent = dot(pick_ref[m], rows).astype(jnp.bfloat16)
        out_ref[:, :capacity, :] = sent.reshape(experts, capacity, width)
    sent = (dot(pick_ref[0], grads_ref[...]) * scale_ref[0]).astype(jnp.bfloat16)
    both_ref[:, capacity:, :] = sent.reshape(experts, capacity, width)


def pack_grads_kernel(grads_ref, pick_ref, scale_ref, out_ref):
    sent = (dot(pick_ref[1], grads_ref[...]) * scale_ref[1]).astype(jnp.bfloat16)
    out_ref[...] = sent.reshape(out_ref.shape)


def forward_parts(rows, gate_0, up_0, gate_1, up_1, gate_ref, up_ref):
    hidden = gate_0.shape[1]
    gate_ref[:, :hidden] = dot(rows, gate_0[...]).astype(jnp.bfloat16)
    gate_ref[:, hidden:] = dot(rows, gate_1[...]).astype(jnp.bfloat16)
    up_ref[:, :hidden] = dot(rows, up_0[...]).astype(jnp.bfloat16)
    up_ref[:, hidden:] = dot(rows, up_1[...]).astype(jnp.bfloat16)


def backward_part(rows, down_0, down_1, hidden_ref):
    hidden = down_0.shape[0]
    hidden_ref[:, :hidden] = dot_last(rows, down_0[...]).astype(jnp.bfloat16)
    hidden_ref[:, hidden:] = dot_last(rows, down_1[...]).astype(jnp.bfloat16)


def both_parts_kernel(
    both_ref, gate_0, up_0, down_0, gate_1, up_1, down_1, gate_ref, up_ref, hidden_ref
):
    sources, twice, width = both_ref.shape
    capacity = twice // 2
    rows = both_ref[:, :capacity, :].reshape(sources * capacity, width)
    forward_parts(rows, gate_0, up_0, gate_1, up_1, gate_ref, up_ref)
    rows = both_ref[:, capacity:, :].reshape(sources * capacity, width)
    backward_part(rows, down_0, down_1, hidden_ref)


def forward_parts_kernel(rows_ref, gate_0, up_0, gate_1, up_1, gate_ref, up_ref):
    rows = rows_ref[...].reshape(gate_ref.shape[0], rows_ref.shape[2])
    forward_parts(rows, gate_0, up_0, gate_1, up_1, gate_ref, up_ref)


def backward_part_kernel(rows_ref, down_0, down_1, hidden_ref):
    rows = rows_ref[...].reshape(hidden_ref.shape[0], rows_ref.shape[2])
    backward_part(rows, down_0, down_1, hidden_ref)


def pieces_kernel(
    gate_own, up_own, hid_own, gate_far, up_far, hid_far, gate_0, up_0, gate_1, up_1, out_ref
):
    sources, capacity, lanes = out_ref.shape
    width = lanes - EXTRA
    count = gate_own.shape[0]
    half = gate_0.shape[1]

    def total(own, far, low):
        return own[:, low : low + half].astype(jnp.float32) + far[:, low : low + half].astype(
            jnp.float32
        )

    piece = inner = 0.0
    for low, gate_w, up_w in ((0, gate_0, up_0), (half, gate_1, up_1)):
        gate = total(gate_own, gate_far, low)
        up = total(up_own, up_far, low)
        hidden = total(hid_own, hid_far, low)
        sigma = jax.nn.sigmoid(gate)
        grad_gate = hidden * up * (sigma * (1.0 + gate * (1.0 - sigma)))
        grad_up = hidden * (gate * sigma)
        inner = inner + jnp.sum(gate * grad_gate + up * grad_up, axis=1, keepdims=True)
        piece = piece + dot_last(grad_gate.astype(jnp.bfloat16), gate_w[...])
        piece = piece + dot_last(grad_up.astype(jnp.bfloat16), up_w[...])
    out_ref[:, :, :width] = piece.astype(jnp.bfloat16).reshape(sources, capacity, width)
    coarse = inner.astype(jnp.bfloat16).astype(jnp.float32)
    lane = lax.broadcasted_iota(jnp.int32, (count, EXTRA), 1)
    extra = jnp.where(lane == 0, coarse, jnp.where(lane == 1, inner - coarse, 0.0))
    out_ref[:, :, width:] = extra.astype(jnp.bfloat16).reshape(sources, capacity, EXTRA)


def combine_kernel(micro):
    def kernel(pieces_ref, incoming_ref, inputs_ref, gain_ref, root_ref, pick_ref, out_ref):
        experts, capacity, lanes = pieces_ref.shape
        width = lanes - EXTRA
        pieces = pieces_ref[...].reshape(experts * capacity, lanes)
        total = dot_first(pick_ref[micro], pieces)
        inner = jnp.sum(total[:, width:], axis=1, keepdims=True)
        root = root_ref[micro]
        normed = normalized(inputs_ref[micro], root)
        scaled = gain_ref[...] * total[:, :width]
        result = incoming_ref[...].astype(jnp.float32) + (scaled - normed * (inner / D)) / root
        out_ref[...] = result.astype(jnp.bfloat16)

    return kernel


def layers(
    saved_inputs, cot_in, loss_grad, expert_ids, route_weights, norm_gain, w_gate, w_up, w_down
):
    section_count = lax.axis_size("section")
    at_last = lax.axis_index("section") == section_count - 1
    experts = lax.axis_size("expert") // 2
    tokens, width = saved_inputs.shape[2:]
    capacity = CAPACITY
    slots = experts * capacity
    hidden = 2 * w_gate.shape[3]
    inputs = saved_inputs[0]
    own = (w_gate[0, 0], w_up[0, 0], w_down[0, 0])

    def like(shape, dtype=jnp.bfloat16):
        return jax.ShapeDtypeStruct(shape, dtype)

    wide = inputs.astype(jnp.float32)
    squares = jnp.sum(wide * wide, axis=2)
    squares = squares + swap(squares)
    root = jnp.sqrt(squares / D + epsilon)[:, :, None]
    pick, scale = call(
        tables_kernel,
        [like((2, slots, tokens)), like((2, slots, 1), jnp.float32)],
        expert_ids[0].transpose(0, 2, 1),
        route_weights[0].transpose(0, 2, 1),
    )
    both, rows_1 = call(
        pack_kernel,
        [like((experts, 2 * capacity, width)), like((experts, capacity, width))],
        inputs,
        cot_in[0],
        norm_gain,
        root,
        pick,
        scale,
    )
    far = [pair_swap(w) for w in own]
    gates = (own[0], own[1], far[0], far[1])
    downs = (own[2], far[2])
    part = like((slots, hidden))

    both = exchange(both)
    rows_1 = exchange(rows_1)
    parts_0 = call(both_parts_kernel, [part] * 3, both, *own, *far)
    parts_1 = call(forward_parts_kernel, [part] * 2, rows_1, *gates)

    def finish(micro, parts, others, incoming):
        pieces = call(
            pieces_kernel, like((experts, capacity, width + EXTRA)), *parts, *others, *gates
        )
        return call(
            combine_kernel(micro),
            like((tokens, width)),
            exchange(pieces),
            incoming,
            inputs,
            norm_gain,
            root,
            pick,
        )

    others_0 = [swap(p) for p in parts_0]
    others_0, parts_1 = lax.optimization_barrier((others_0, parts_1))
    first_grads = finish(0, parts_0, others_0, cot_in[0])
    others_1 = [swap(p) for p in parts_1]
    pairs = [(i, i - 1) for i in range(1, section_count)]
    passed = lax.ppermute(first_grads, "section", pairs)
    incoming = jnp.where(at_last, loss_grad, passed)
    grads_1 = exchange(
        call(pack_grads_kernel, like((experts, capacity, width)), incoming, pick, scale),
    )
    hidden_1 = call(backward_part_kernel, part, grads_1, *downs)
    second_grads = finish(1, [*parts_1, hidden_1], [*others_1, swap(hidden_1)], incoming)
    return jnp.stack([first_grads, second_grads])[None]


def solution(mesh):
    in_specs = (
        P("section", None, "expert", "tensor"),
        P("section", "expert", "tensor"),
        P("expert", "tensor"),
        P("section", None, "expert", None),
        P("section", None, "expert", None),
        P("section", "tensor"),
        P("section", "expert", "tensor", None),
        P("section", "expert", "tensor", None),
        P("section", "expert", None, "tensor"),
    )
    out_specs = P("section", None, "expert", "tensor")
    return jax.shard_map(layers, mesh=mesh, in_specs=in_specs, out_specs=out_specs, check_vma=False)
```

```python
import jax
import jax.numpy as jnp
from jax import lax
from jax.experimental import pallas as pl
from jax.experimental.pallas import tpu as pltpu
from jax.sharding import PartitionSpec as P

D = 2048
epsilon = 1e-06
VMEM_LIMIT = 48 * 1024 * 1024
EXTRA = 128
CAPACITY = 24


def call(kernel, out_shape, *operands):
    def spec():
        return pl.BlockSpec(memory_space=pltpu.VMEM)

    several = isinstance(out_shape, (list, tuple))
    return pl.pallas_call(
        kernel,
        out_shape=out_shape,
        in_specs=[spec() for _ in operands],
        out_specs=[spec() for _ in out_shape] if several else spec(),
        compiler_params=pltpu.CompilerParams(vmem_limit_bytes=VMEM_LIMIT),
    )(*operands)


def dot(left, right):
    return jnp.dot(left, right, preferred_element_type=jnp.float32)


def dot_last(left, right):
    return lax.dot_general(
        left, right, (((1,), (1,)), ((), ())), preferred_element_type=jnp.float32
    )


def dot_first(left, right):
    return lax.dot_general(
        left, right, (((0,), (0,)), ((), ())), preferred_element_type=jnp.float32
    )


def swap(array):
    return lax.ppermute(array, "tensor", [(0, 1), (1, 0)])


def pair_swap(array):
    pairs = [(i, i ^ 1) for i in range(lax.axis_size("expert"))]
    return lax.ppermute(array, "expert", pairs)


def exchange(array):
    count = lax.axis_size("expert")
    groups = [list(range(parity, count, 2)) for parity in range(2)]
    return lax.all_to_all(
        array, "expert", split_axis=0, concat_axis=0, tiled=True, axis_index_groups=groups
    )


def tables_kernel(ids_ref, weights_ref, pick_ref, scale_ref):
    micros, per_token, tokens = ids_ref.shape
    slots = pick_ref.shape[1]
    experts = slots // CAPACITY
    capacity = CAPACITY
    row = lax.broadcasted_iota(jnp.int32, (tokens, tokens), 0)
    col = lax.broadcasted_iota(jnp.int32, (tokens, tokens), 1)
    earlier = (row < col).astype(jnp.bfloat16)
    expert = lax.broadcasted_iota(jnp.int32, (experts, tokens), 0)
    slot = lax.broadcasted_iota(jnp.int32, (capacity, tokens), 0).astype(jnp.float32)
    for m in range(micros):
        member = jnp.zeros((experts, tokens), jnp.float32)
        weight = jnp.zeros((experts, tokens), jnp.float32)
        for k in range(per_token):
            hit = ids_ref[m, k : k + 1, :] == expert
            member = jnp.where(hit, 1.0, member)
            weight = jnp.where(hit, weights_ref[m, k : k + 1, :], weight)
        before = dot(member.astype(jnp.bfloat16), earlier)
        place = jnp.where(member > 0.0, before, -1.0)
        for e in range(experts):
            hit = slot == place[e : e + 1, :]
            pick_ref[m, e * capacity : (e + 1) * capacity, :] = jnp.where(hit, 1.0, 0.0).astype(
                jnp.bfloat16
            )
            scale_ref[m, e * capacity : (e + 1) * capacity, :] = jnp.sum(
                jnp.where(hit, weight[e : e + 1, :], 0.0), axis=1, keepdims=True
            )


def normalized(inputs, root):
    return inputs.astype(jnp.float32) / root


def pack_kernel(inputs_ref, grads_ref, gain_ref, root_ref, pick_ref, scale_ref, out_ref):
    experts, thrice, width = out_ref.shape
    capacity = thrice // 3
    gain = gain_ref[...]
    for m in (0, 1):
        rows = (normalized(inputs_ref[m], root_ref[m]) * gain).astype(jnp.bfloat16)
        sent = dot(pick_ref[m], rows).astype(jnp.bfloat16)
        low = 2 * m * capacity
        out_ref[:, low : low + capacity, :] = sent.reshape(experts, capacity, width)
    sent = (dot(pick_ref[0], grads_ref[...]) * scale_ref[0]).astype(jnp.bfloat16)
    out_ref[:, capacity : 2 * capacity, :] = sent.reshape(experts, capacity, width)


def pack_grads_kernel(grads_ref, pick_ref, scale_ref, out_ref):
    sent = (dot(pick_ref[1], grads_ref[...]) * scale_ref[1]).astype(jnp.bfloat16)
    out_ref[...] = sent.reshape(out_ref.shape)


def forward_parts(rows, gate_0, up_0, gate_1, up_1, gate_ref, up_ref):
    hidden = gate_0.shape[1]
    gate_ref[:, :hidden] = dot(rows, gate_0[...]).astype(jnp.bfloat16)
    gate_ref[:, hidden:] = dot(rows, gate_1[...]).astype(jnp.bfloat16)
    up_ref[:, :hidden] = dot(rows, up_0[...]).astype(jnp.bfloat16)
    up_ref[:, hidden:] = dot(rows, up_1[...]).astype(jnp.bfloat16)


def backward_part(rows, down_0, down_1, hidden_ref):
    hidden = down_0.shape[0]
    hidden_ref[:, :hidden] = dot_last(rows, down_0[...]).astype(jnp.bfloat16)
    hidden_ref[:, hidden:] = dot_last(rows, down_1[...]).astype(jnp.bfloat16)


def both_parts_kernel(
    rows_ref, gate_0, up_0, down_0, gate_1, up_1, down_1, gate_ref, up_ref, hidden_ref
):
    sources, thrice, width = rows_ref.shape
    capacity = thrice // 3
    rows = rows_ref[:, :capacity, :].reshape(sources * capacity, width)
    forward_parts(rows, gate_0, up_0, gate_1, up_1, gate_ref, up_ref)
    rows = rows_ref[:, capacity : 2 * capacity, :].reshape(sources * capacity, width)
    backward_part(rows, down_0, down_1, hidden_ref)


def forward_parts_kernel(rows_ref, gate_0, up_0, gate_1, up_1, gate_ref, up_ref):
    _, thrice, width = rows_ref.shape
    low = 2 * thrice // 3
    rows = rows_ref[:, low:, :].reshape(gate_ref.shape[0], width)
    forward_parts(rows, gate_0, up_0, gate_1, up_1, gate_ref, up_ref)


def backward_part_kernel(rows_ref, down_0, down_1, hidden_ref):
    rows = rows_ref[...].reshape(hidden_ref.shape[0], rows_ref.shape[2])
    backward_part(rows, down_0, down_1, hidden_ref)


def pieces_kernel(
    gate_own, up_own, hid_own, gate_far, up_far, hid_far, gate_0, up_0, gate_1, up_1, out_ref
):
    sources, capacity, lanes = out_ref.shape
    width = lanes - EXTRA
    count = gate_own.shape[0]
    half = gate_0.shape[1]

    def total(own, far, low):
        return own[:, low : low + half].astype(jnp.float32) + far[:, low : low + half].astype(
            jnp.float32
        )

    piece = inner = 0.0
    for low, gate_w, up_w in ((0, gate_0, up_0), (half, gate_1, up_1)):
        gate = total(gate_own, gate_far, low)
        up = total(up_own, up_far, low)
        hidden = total(hid_own, hid_far, low)
        sigma = jax.nn.sigmoid(gate)
        grad_gate = hidden * up * (sigma * (1.0 + gate * (1.0 - sigma)))
        grad_up = hidden * (gate * sigma)
        inner = inner + jnp.sum(gate * grad_gate + up * grad_up, axis=1, keepdims=True)
        piece = piece + dot_last(grad_gate.astype(jnp.bfloat16), gate_w[...])
        piece = piece + dot_last(grad_up.astype(jnp.bfloat16), up_w[...])
    out_ref[:, :, :width] = piece.astype(jnp.bfloat16).reshape(sources, capacity, width)
    coarse = inner.astype(jnp.bfloat16).astype(jnp.float32)
    lane = lax.broadcasted_iota(jnp.int32, (count, EXTRA), 1)
    extra = jnp.where(lane == 0, coarse, jnp.where(lane == 1, inner - coarse, 0.0))
    out_ref[:, :, width:] = extra.astype(jnp.bfloat16).reshape(sources, capacity, EXTRA)


def combine_kernel(micro):
    def kernel(pieces_ref, incoming_ref, inputs_ref, gain_ref, root_ref, pick_ref, out_ref):
        experts, capacity, lanes = pieces_ref.shape
        width = lanes - EXTRA
        pieces = pieces_ref[...].reshape(experts * capacity, lanes)
        total = dot_first(pick_ref[micro], pieces)
        inner = jnp.sum(total[:, width:], axis=1, keepdims=True)
        root = root_ref[micro]
        normed = normalized(inputs_ref[micro], root)
        scaled = gain_ref[...] * total[:, :width]
        result = incoming_ref[...].astype(jnp.float32) + (scaled - normed * (inner / D)) / root
        out_ref[...] = result.astype(jnp.bfloat16)

    return kernel


def layers(
    saved_inputs, cot_in, loss_grad, expert_ids, route_weights, norm_gain, w_gate, w_up, w_down
):
    section_count = lax.axis_size("section")
    at_last = lax.axis_index("section") == section_count - 1
    experts = lax.axis_size("expert") // 2
    tokens, width = saved_inputs.shape[2:]
    capacity = CAPACITY
    slots = experts * capacity
    hidden = 2 * w_gate.shape[3]
    inputs = saved_inputs[0]
    own = (w_gate[0, 0], w_up[0, 0], w_down[0, 0])

    def like(shape, dtype=jnp.bfloat16):
        return jax.ShapeDtypeStruct(shape, dtype)

    wide = inputs.astype(jnp.float32)
    squares = jnp.sum(wide * wide, axis=2)
    squares = squares + swap(squares)
    root = jnp.sqrt(squares / D + epsilon)[:, :, None]
    pick, scale = call(
        tables_kernel,
        [like((2, slots, tokens)), like((2, slots, 1), jnp.float32)],
        expert_ids[0].transpose(0, 2, 1),
        route_weights[0].transpose(0, 2, 1),
    )
    rows = call(
        pack_kernel,
        like((experts, 3 * capacity, width)),
        inputs,
        cot_in[0],
        norm_gain,
        root,
        pick,
        scale,
    )
    far = [pair_swap(w) for w in own]
    gates = (own[0], own[1], far[0], far[1])
    downs = (own[2], far[2])
    part = like((slots, hidden))

    rows = exchange(rows)
    parts_0 = call(both_parts_kernel, [part] * 3, rows, *own, *far)
    parts_1 = call(forward_parts_kernel, [part] * 2, rows, *gates)

    def finish(micro, parts, others, incoming):
        pieces = call(
            pieces_kernel, like((experts, capacity, width + EXTRA)), *parts, *others, *gates
        )
        return call(
            combine_kernel(micro),
            like((tokens, width)),
            exchange(pieces),
            incoming,
            inputs,
            norm_gain,
            root,
            pick,
        )

    others_0 = [swap(p) for p in parts_0]
    others_0, parts_1 = lax.optimization_barrier((others_0, parts_1))
    first_grads = finish(0, parts_0, others_0, cot_in[0])
    others_1 = [swap(p) for p in parts_1]
    pairs = [(i, i - 1) for i in range(1, section_count)]
    passed = lax.ppermute(first_grads, "section", pairs)
    incoming = jnp.where(at_last, loss_grad, passed)
    grads_1 = exchange(
        call(pack_grads_kernel, like((experts, capacity, width)), incoming, pick, scale),
    )
    hidden_1 = call(backward_part_kernel, part, grads_1, *downs)
    second_grads = finish(1, [*parts_1, hidden_1], [*others_1, swap(hidden_1)], incoming)
    return jnp.stack([first_grads, second_grads])[None]


def solution(mesh):
    in_specs = (
        P("section", None, "expert", "tensor"),
        P("section", "expert", "tensor"),
        P("expert", "tensor"),
        P("section", None, "expert", None),
        P("section", None, "expert", None),
        P("section", "tensor"),
        P("section", "expert", "tensor", None),
        P("section", "expert", "tensor", None),
        P("section", "expert", None, "tensor"),
    )
    out_specs = P("section", None, "expert", "tensor")
    return jax.shard_map(layers, mesh=mesh, in_specs=in_specs, out_specs=out_specs, check_vma=False)
```

```python
import jax
import jax.numpy as jnp
from jax import lax
from jax.experimental import pallas as pl
from jax.experimental.pallas import tpu as pltpu
from jax.sharding import PartitionSpec as P

D = 2048
epsilon = 1e-06
VMEM_LIMIT = 48 * 1024 * 1024
EXTRA = 128
SHARE = 12


def call(kernel, out_shape, *operands, scalar=None):
    def spec():
        return pl.BlockSpec(memory_space=pltpu.VMEM)

    several = isinstance(out_shape, (list, tuple))
    in_specs = [spec() for _ in operands]
    if scalar is not None:
        in_specs = [pl.BlockSpec(memory_space=pltpu.SMEM), *in_specs]
        operands = (scalar, *operands)
    return pl.pallas_call(
        kernel,
        out_shape=out_shape,
        in_specs=in_specs,
        out_specs=[spec() for _ in out_shape] if several else spec(),
        compiler_params=pltpu.CompilerParams(vmem_limit_bytes=VMEM_LIMIT),
    )(*operands)


def dot(left, right):
    return jnp.dot(left, right, preferred_element_type=jnp.float32)


def dot_last(left, right):
    return lax.dot_general(
        left, right, (((1,), (1,)), ((), ())), preferred_element_type=jnp.float32
    )


def dot_first(left, right):
    return lax.dot_general(
        left, right, (((0,), (0,)), ((), ())), preferred_element_type=jnp.float32
    )


def swap(array):
    return lax.ppermute(array, "tensor", [(0, 1), (1, 0)])


def pair_swap(array):
    pairs = [(i, i ^ 1) for i in range(lax.axis_size("expert"))]
    return lax.ppermute(array, "expert", pairs)


def diagonal_swap(array):
    count = lax.axis_size("expert")
    pairs = [(t * count + i, (1 - t) * count + (i ^ 1)) for t in (0, 1) for i in range(count)]
    return lax.ppermute(array, ("tensor", "expert"), pairs)


def exchange(array):
    count = lax.axis_size("expert")
    groups = [
        [t * count + i for t in (0, 1) for i in range(parity, count, 2)] for parity in (0, 1)
    ]
    return lax.all_to_all(
        array,
        ("tensor", "expert"),
        split_axis=0,
        concat_axis=0,
        tiled=True,
        axis_index_groups=groups,
    )


def tables_kernel(ids_ref, weights_ref, pick_a_ref, pick_b_ref, scale_a_ref, scale_b_ref):
    micros, per_token, tokens = ids_ref.shape
    experts = pick_a_ref.shape[1] // 16
    row = lax.broadcasted_iota(jnp.int32, (tokens, tokens), 0)
    col = lax.broadcasted_iota(jnp.int32, (tokens, tokens), 1)
    earlier = (row < col).astype(jnp.bfloat16)
    expert = lax.broadcasted_iota(jnp.int32, (experts, tokens), 0)
    line = lax.broadcasted_iota(jnp.int32, (8, tokens), 0)
    slot_a = line.astype(jnp.float32)
    slot_b = jnp.where(line < 4, line + 8, line + 4).astype(jnp.float32)

    def ones(hit):
        return jnp.where(hit, 1.0, 0.0).astype(jnp.bfloat16)

    for m in range(micros):
        member = jnp.zeros((experts, tokens), jnp.float32)
        weight = jnp.zeros((experts, tokens), jnp.float32)
        for k in range(per_token):
            hit = ids_ref[m, k : k + 1, :] == expert
            member = jnp.where(hit, 1.0, member)
            weight = jnp.where(hit, weights_ref[m, k : k + 1, :], weight)
        before = dot(member.astype(jnp.bfloat16), earlier)
        place = jnp.where(member > 0.0, before, -1.0)
        for rank in range(2):
            for e in range(experts):
                low = (rank * experts + e) * 8
                here = place[e : e + 1, :] - float(rank * SHARE)
                hit_a = slot_a == here
                hit_b = slot_b == here
                pick_a_ref[m, low : low + 8, :] = ones(hit_a)
                pick_b_ref[m, low : low + 8, :tokens] = ones(hit_b & (line < 4))
                pick_b_ref[m, low : low + 8, tokens:] = ones(hit_b & (line >= 4))
                for hit, ref in ((hit_a, scale_a_ref), (hit_b, scale_b_ref)):
                    ref[m, low : low + 8, :] = jnp.sum(
                        jnp.where(hit, weight[e : e + 1, :], 0.0), axis=1, keepdims=True
                    )


def normalized(inputs, root):
    return inputs.astype(jnp.float32) / root


def put(rows, pick_a, pick_b, scales, out_ref, low):
    peers = out_ref.shape[0]
    width = rows.shape[1]
    half = width // 2
    first = dot(pick_a, rows)
    second = dot(pick_b, jnp.concatenate([rows[:, :half], rows[:, half:]], axis=0))
    if scales is not None:
        first = first * scales[0]
        second = second * scales[1]
    out_ref[:, low : low + 8, :width] = first.astype(jnp.bfloat16).reshape(peers, 8, width)
    out_ref[:, low : low + 8, width:] = second.astype(jnp.bfloat16).reshape(peers, 8, half)


def pack_kernel(
    inputs_ref, grads_ref, gain_ref, root_ref, pick_a, pick_b, scale_a, scale_b, out_ref
):
    gain = gain_ref[...]
    for m in (0, 1):
        rows = (normalized(inputs_ref[m], root_ref[m]) * gain).astype(jnp.bfloat16)
        put(rows, pick_a[m], pick_b[m], None, out_ref, 16 * m)
    put(grads_ref[...], pick_a[0], pick_b[0], (scale_a[0], scale_b[0]), out_ref, 8)


def pack_grads_kernel(grads_ref, pick_a, pick_b, scale_a, scale_b, out_ref):
    put(grads_ref[...], pick_a[1], pick_b[1], (scale_a[1], scale_b[1]), out_ref, 0)


def take(ref, start, low, sources):
    part = ref[pl.ds(start, sources), low : low + 8, :]
    width = 2 * part.shape[2] // 3
    tail = part[:, :, width:]
    upper = lax.broadcasted_iota(jnp.int32, tail.shape, 1) < 4
    zero = jnp.zeros_like(tail)
    tail = jnp.concatenate([jnp.where(upper, tail, zero), jnp.where(upper, zero, tail)], axis=2)
    count = sources * 8
    return jnp.concatenate(
        [part[:, :, :width].reshape(count, width), tail.reshape(count, width)], axis=0
    )


def joined(values):
    count = values.shape[0] // 2
    tail = values[count:].reshape(count // 8, 8, values.shape[1])
    tail = tail + pltpu.roll(tail, 4, 1)
    return jnp.concatenate([values[:count], tail.reshape(count, values.shape[1])], axis=0)


def forward_kernel(low):
    def kernel(rank_ref, rows_ref, *refs):
        weights, (gate_ref, up_ref) = refs[:-2], refs[-2:]
        sources = rows_ref.shape[0] // 2
        rank = rank_ref[0]
        parts = [take(rows_ref, place * sources, low, sources) for place in (rank, 1 - rank)]
        half = weights[0].shape[1]
        for kind, out_ref in ((0, gate_ref), (1, up_ref)):
            for f in range(2):
                total = dot(parts[0], weights[2 * f + kind][...])
                total = total + dot(parts[1], weights[4 + 2 * f + kind][...])
                out_ref[:, f * half : (f + 1) * half] = joined(total)

    return kernel


def backward_kernel(low):
    def kernel(rank_ref, grads_ref, gate_ref, up_ref, *refs):
        weights, downs, out_ref = refs[:8], refs[8:12], refs[12]
        peers, _, _ = out_ref.shape
        sources = peers // 2
        count = sources * 8
        half = weights[0].shape[1]
        width = weights[0].shape[0]
        rank = rank_ref[0]
        starts = (rank * sources, (1 - rank) * sources)
        parts = [take(grads_ref, start, low, sources) for start in starts]
        pieces = [0.0, 0.0]
        inner = 0.0
        for f in range(2):
            hidden = dot_last(parts[0], downs[f][...]) + dot_last(parts[1], downs[2 + f][...])
            hidden = joined(hidden)
            gate = gate_ref[:, f * half : (f + 1) * half]
            up = up_ref[:, f * half : (f + 1) * half]
            sigma = jax.nn.sigmoid(gate)
            grad_gate = hidden * up * (sigma * (1.0 + gate * (1.0 - sigma)))
            grad_up = hidden * (gate * sigma)
            inner = inner + jnp.sum(gate * grad_gate + up * grad_up, axis=1, keepdims=True)
            grad_gate = grad_gate.astype(jnp.bfloat16)
            grad_up = grad_up.astype(jnp.bfloat16)
            for i in range(2):
                pieces[i] = pieces[i] + dot_last(grad_gate, weights[4 * i + 2 * f][...])
                pieces[i] = pieces[i] + dot_last(grad_up, weights[4 * i + 2 * f + 1][...])
        coarse = inner.astype(jnp.bfloat16).astype(jnp.float32)
        fine = inner - coarse
        lane = lax.broadcasted_iota(jnp.int32, (count, EXTRA), 1)
        extra = jnp.zeros((count, EXTRA), jnp.float32)
        for place, column in enumerate(
            (coarse[:count], fine[:count], coarse[count:], fine[count:])
        ):
            extra = jnp.where(lane == place, column, extra)
        extra = extra.astype(jnp.bfloat16).reshape(sources, 8, EXTRA)
        upper = lax.broadcasted_iota(jnp.int32, (sources, 8, width // 2), 1) < 4
        for piece, start in zip(pieces, starts):
            tail = piece[count:].reshape(sources, 8, width)
            tail = jnp.where(upper, tail[:, :, : width // 2], tail[:, :, width // 2 :])
            here = pl.ds(start, sources)
            out_ref[here, :, :width] = (
                piece[:count].astype(jnp.bfloat16).reshape(sources, 8, width)
            )
            out_ref[here, :, width : width + EXTRA] = extra
            out_ref[here, :, width + EXTRA :] = tail.astype(jnp.bfloat16)

    return kernel


def combine_kernel(micro):
    def kernel(pieces_ref, incoming_ref, inputs_ref, gain_ref, root_ref, pick_a, pick_b, out_ref):
        peers, eight, lanes = pieces_ref.shape
        tokens, width = out_ref.shape
        pieces = pieces_ref[...].reshape(peers * eight, lanes)
        first = dot_first(pick_a[micro], pieces[:, : width + EXTRA])
        second = dot_first(pick_b[micro], pieces[:, width:])
        lane = lax.broadcasted_iota(jnp.int32, (tokens, EXTRA), 1)
        inner = jnp.where(lane < 2, first[:, width:], 0.0) + jnp.where(
            (lane >= 2) & (lane < 4), second[:tokens, :EXTRA], 0.0
        )
        inner = jnp.sum(inner, axis=1, keepdims=True)
        total = first[:, :width] + jnp.concatenate(
            [second[:tokens, EXTRA:], second[tokens:, EXTRA:]], axis=1
        )
        root = root_ref[micro]
        normed = normalized(inputs_ref[micro], root)
        scaled = gain_ref[...] * total
        result = incoming_ref[...].astype(jnp.float32) + (scaled - normed * (inner / D)) / root
        out_ref[...] = result.astype(jnp.bfloat16)

    return kernel


def layers(
    saved_inputs, cot_in, loss_grad, expert_ids, route_weights, norm_gain, w_gate, w_up, w_down
):
    section_count = lax.axis_size("section")
    at_last = lax.axis_index("section") == section_count - 1
    rank = lax.axis_index("tensor").astype(jnp.int32)[None]
    experts = lax.axis_size("expert") // 2
    peers = 2 * experts
    tokens, width = saved_inputs.shape[2:]
    lanes = 3 * width // 2
    hidden = 2 * w_gate.shape[3]
    inputs = saved_inputs[0]
    own = (w_gate[0, 0], w_up[0, 0], w_down[0, 0])

    def like(shape, dtype=jnp.bfloat16):
        return jax.ShapeDtypeStruct(shape, dtype)

    wide = inputs.astype(jnp.float32)
    squares = jnp.sum(wide * wide, axis=2)
    squares = squares + swap(squares)
    root = jnp.sqrt(squares / D + epsilon)[:, :, None]
    slots = peers * 8
    tables = call(
        tables_kernel,
        [
            like((2, slots, tokens)),
            like((2, slots, 2 * tokens)),
            like((2, slots, 1), jnp.float32),
            like((2, slots, 1), jnp.float32),
        ],
        expert_ids[0].transpose(0, 2, 1),
        route_weights[0].transpose(0, 2, 1),
    )
    rows = call(
        pack_kernel, like((peers, 24, lanes)), inputs, cot_in[0], norm_gain, root, *tables
    )
    rows = exchange(rows)
    cross = [diagonal_swap(w) for w in own]
    pair = [pair_swap(w) for w in own]
    far = [pair_swap(w) for w in cross]
    quad = (own, pair, far, cross)
    gates = [w for part in quad for w in part[:2]]
    downs = [part[2] for part in quad]

    def forward(micro):
        return call(
            forward_kernel(16 * micro),
            [like((2 * experts * 8, hidden), jnp.float32)] * 2,
            rows,
            *gates,
            scalar=rank,
        )

    def finish(micro, sums, grads, low, incoming):
        pieces = call(
            backward_kernel(low),
            like((peers, 8, lanes + EXTRA)),
            grads,
            *sums,
            *gates,
            *downs,
            scalar=rank,
        )
        return call(
            combine_kernel(micro),
            like((tokens, width)),
            exchange(pieces),
            incoming,
            inputs,
            norm_gain,
            root,
            *tables[:2],
        )

    first_grads = finish(0, forward(0), rows, 8, cot_in[0])
    sums_1 = forward(1)
    pairs = [(i, i - 1) for i in range(1, section_count)]
    passed = lax.ppermute(first_grads, "section", pairs)
    incoming = jnp.where(at_last, loss_grad, passed)
    grads_1 = exchange(call(pack_grads_kernel, like((peers, 8, lanes)), incoming, *tables))
    second_grads = finish(1, sums_1, grads_1, 0, incoming)
    return jnp.stack([first_grads, second_grads])[None]


def solution(mesh):
    in_specs = (
        P("section", None, "expert", "tensor"),
        P("section", "expert", "tensor"),
        P("expert", "tensor"),
        P("section", None, "expert", None),
        P("section", None, "expert", None),
        P("section", "tensor"),
        P("section", "expert", "tensor", None),
        P("section", "expert", "tensor", None),
        P("section", "expert", None, "tensor"),
    )
    out_specs = P("section", None, "expert", "tensor")
    return jax.shard_map(layers, mesh=mesh, in_specs=in_specs, out_specs=out_specs, check_vma=False)
```

```python
import jax
import jax.numpy as jnp
from jax import lax
from jax.experimental import pallas as pl
from jax.experimental.pallas import tpu as pltpu
from jax.sharding import PartitionSpec as P

D = 2048
epsilon = 1e-06
LARGE = 24 * 1024 * 1024
SMALL = 12 * 1024 * 1024
EXTRA = 128
SHARE = 12


def call(kernel, out_shape, *operands, scalar=None, outside=(), scratch=()):
    def spec():
        return pl.BlockSpec(memory_space=pltpu.VMEM)

    several = isinstance(out_shape, (list, tuple))
    in_specs = [spec() for _ in operands]
    in_specs += [pl.BlockSpec(memory_space=pltpu.HBM) for _ in outside]
    operands = (*operands, *outside)
    if scalar is not None:
        in_specs = [pl.BlockSpec(memory_space=pltpu.SMEM), *in_specs]
        operands = (scalar, *operands)
    return pl.pallas_call(
        kernel,
        out_shape=out_shape,
        in_specs=in_specs,
        out_specs=[spec() for _ in out_shape] if several else spec(),
        scratch_shapes=scratch,
        compiler_params=pltpu.CompilerParams(
            vmem_limit_bytes=SMALL if scalar is None else LARGE
        ),
    )(*operands)


def dot(left, right):
    return jnp.dot(left, right, preferred_element_type=jnp.float32)


def dot_last(left, right):
    return lax.dot_general(
        left, right, (((1,), (1,)), ((), ())), preferred_element_type=jnp.float32
    )


def dot_first(left, right):
    return lax.dot_general(
        left, right, (((0,), (0,)), ((), ())), preferred_element_type=jnp.float32
    )


def swap(array):
    return lax.ppermute(array, "tensor", [(0, 1), (1, 0)])


def pair_swap(array):
    pairs = [(i, i ^ 1) for i in range(lax.axis_size("expert"))]
    return lax.ppermute(array, "expert", pairs)


def diagonal_swap(array):
    count = lax.axis_size("expert")
    pairs = [(t * count + i, (1 - t) * count + (i ^ 1)) for t in (0, 1) for i in range(count)]
    return lax.ppermute(array, ("tensor", "expert"), pairs)


def exchange(array):
    count = lax.axis_size("expert")
    groups = [
        [t * count + i for t in (0, 1) for i in range(parity, count, 2)] for parity in (0, 1)
    ]
    return lax.all_to_all(
        array,
        ("tensor", "expert"),
        split_axis=0,
        concat_axis=0,
        tiled=True,
        axis_index_groups=groups,
    )


def tables_kernel(ids_ref, weights_ref, pick_a_ref, pick_b_ref, scale_a_ref, scale_b_ref):
    micros, per_token, tokens = ids_ref.shape
    experts = pick_a_ref.shape[1] // 16
    row = lax.broadcasted_iota(jnp.int32, (tokens, tokens), 0)
    col = lax.broadcasted_iota(jnp.int32, (tokens, tokens), 1)
    earlier = (row < col).astype(jnp.bfloat16)
    expert = lax.broadcasted_iota(jnp.int32, (experts, tokens), 0)
    line = lax.broadcasted_iota(jnp.int32, (8, tokens), 0)
    slot_a = line.astype(jnp.float32)
    slot_b = jnp.where(line < 4, line + 8, line + 4).astype(jnp.float32)

    def ones(hit):
        return jnp.where(hit, 1.0, 0.0).astype(jnp.bfloat16)

    for m in range(micros):
        member = jnp.zeros((experts, tokens), jnp.float32)
        weight = jnp.zeros((experts, tokens), jnp.float32)
        for k in range(per_token):
            hit = ids_ref[m, k : k + 1, :] == expert
            member = jnp.where(hit, 1.0, member)
            weight = jnp.where(hit, weights_ref[m, k : k + 1, :], weight)
        before = dot(member.astype(jnp.bfloat16), earlier)
        place = jnp.where(member > 0.0, before, -1.0)
        for rank in range(2):
            for e in range(experts):
                low = (rank * experts + e) * 8
                here = place[e : e + 1, :] - float(rank * SHARE)
                hit_a = slot_a == here
                hit_b = slot_b == here
                pick_a_ref[m, low : low + 8, :] = ones(hit_a)
                pick_b_ref[m, low : low + 8, :tokens] = ones(hit_b & (line < 4))
                pick_b_ref[m, low : low + 8, tokens:] = ones(hit_b & (line >= 4))
                for hit, ref in ((hit_a, scale_a_ref), (hit_b, scale_b_ref)):
                    ref[m, low : low + 8, :] = jnp.sum(
                        jnp.where(hit, weight[e : e + 1, :], 0.0), axis=1, keepdims=True
                    )


def normalized(inputs, root):
    return inputs.astype(jnp.float32) / root


def put(rows, pick_a, pick_b, scales, out_ref, low):
    peers = out_ref.shape[0]
    width = rows.shape[1]
    half = width // 2
    first = dot(pick_a, rows)
    second = dot(pick_b, jnp.concatenate([rows[:, :half], rows[:, half:]], axis=0))
    if scales is not None:
        first = first * scales[0]
        second = second * scales[1]
    out_ref[:, low : low + 8, :width] = first.astype(jnp.bfloat16).reshape(peers, 8, width)
    out_ref[:, low : low + 8, width:] = second.astype(jnp.bfloat16).reshape(peers, 8, half)


def pack_kernel(
    inputs_ref, grads_ref, gain_ref, root_ref, pick_a, pick_b, scale_a, scale_b, out_ref
):
    gain = gain_ref[...]
    for m in (0, 1):
        rows = (normalized(inputs_ref[m], root_ref[m]) * gain).astype(jnp.bfloat16)
        put(rows, pick_a[m], pick_b[m], None, out_ref, 16 * m)
    put(grads_ref[...], pick_a[0], pick_b[0], (scale_a[0], scale_b[0]), out_ref, 8)


def pack_grads_kernel(grads_ref, pick_a, pick_b, scale_a, scale_b, out_ref):
    put(grads_ref[...], pick_a[1], pick_b[1], (scale_a[1], scale_b[1]), out_ref, 0)


def take(ref, start, low, sources):
    part = ref[pl.ds(start, sources), low : low + 8, :]
    width = 2 * part.shape[2] // 3
    tail = part[:, :, width:]
    upper = lax.broadcasted_iota(jnp.int32, tail.shape, 1) < 4
    zero = jnp.zeros_like(tail)
    tail = jnp.concatenate([jnp.where(upper, tail, zero), jnp.where(upper, zero, tail)], axis=2)
    count = sources * 8
    return jnp.concatenate(
        [part[:, :, :width].reshape(count, width), tail.reshape(count, width)], axis=0
    )


def joined(values):
    count = values.shape[0] // 2
    tail = values[count:].reshape(count // 8, 8, values.shape[1])
    tail = tail + pltpu.roll(tail, 4, 1)
    return jnp.concatenate([values[:count], tail.reshape(count, values.shape[1])], axis=0)


def forward_kernel(low):
    def kernel(rank_ref, rows_ref, *refs):
        weights, (gate_ref, up_ref) = refs[:-2], refs[-2:]
        sources = rows_ref.shape[0] // 2
        rank = rank_ref[0]
        parts = [take(rows_ref, place * sources, low, sources) for place in (rank, 1 - rank)]
        half = weights[0].shape[1]
        for kind, out_ref in ((0, gate_ref), (1, up_ref)):
            for f in range(2):
                total = dot(parts[0], weights[2 * f + kind][...])
                total = total + dot(parts[1], weights[4 + 2 * f + kind][...])
                out_ref[:, f * half : (f + 1) * half] = joined(total)

    return kernel


def backward_kernel(low):
    def kernel(rank_ref, grads_ref, gate_ref, up_ref, *refs):
        near, remote, (out_ref, gates_ref, downs_ref, signals) = refs[:3], refs[3:12], refs[12:]
        weights = [near[0], near[1], *(gates_ref.at[i] for i in range(6))]
        downs = [near[2], *(downs_ref.at[i] for i in range(3))]
        copies = [
            pltpu.make_async_copy(source, target, signals.at[i])
            for i, (source, target) in enumerate(zip(remote, [*downs[1:], *weights[2:]]))
        ]
        for copy in copies:
            copy.start()
        peers, _, _ = out_ref.shape
        sources = peers // 2
        count = sources * 8
        half = weights[0].shape[1]
        width = weights[0].shape[0]
        rank = rank_ref[0]
        starts = (rank * sources, (1 - rank) * sources)
        parts = [take(grads_ref, start, low, sources) for start in starts]
        pieces = [0.0, 0.0]
        inner = 0.0
        for copy in copies[:3]:
            copy.wait()
        for f in range(2):
            hidden = dot_last(parts[0], downs[f][...]) + dot_last(parts[1], downs[2 + f][...])
            hidden = joined(hidden)
            gate = gate_ref[:, f * half : (f + 1) * half]
            up = up_ref[:, f * half : (f + 1) * half]
            sigma = jax.nn.sigmoid(gate)
            grad_gate = hidden * up * (sigma * (1.0 + gate * (1.0 - sigma)))
            grad_up = hidden * (gate * sigma)
            inner = inner + jnp.sum(gate * grad_gate + up * grad_up, axis=1, keepdims=True)
            grad_gate = grad_gate.astype(jnp.bfloat16)
            grad_up = grad_up.astype(jnp.bfloat16)
            if f == 0:
                for copy in copies[3:]:
                    copy.wait()
            for i in range(2):
                pieces[i] = pieces[i] + dot_last(grad_gate, weights[4 * i + 2 * f][...])
                pieces[i] = pieces[i] + dot_last(grad_up, weights[4 * i + 2 * f + 1][...])
        coarse = inner.astype(jnp.bfloat16).astype(jnp.float32)
        fine = inner - coarse
        lane = lax.broadcasted_iota(jnp.int32, (count, EXTRA), 1)
        extra = jnp.zeros((count, EXTRA), jnp.float32)
        for place, column in enumerate(
            (coarse[:count], fine[:count], coarse[count:], fine[count:])
        ):
            extra = jnp.where(lane == place, column, extra)
        extra = extra.astype(jnp.bfloat16).reshape(sources, 8, EXTRA)
        upper = lax.broadcasted_iota(jnp.int32, (sources, 8, width // 2), 1) < 4
        for piece, start in zip(pieces, starts):
            tail = piece[count:].reshape(sources, 8, width)
            tail = jnp.where(upper, tail[:, :, : width // 2], tail[:, :, width // 2 :])
            here = pl.ds(start, sources)
            out_ref[here, :, :width] = (
                piece[:count].astype(jnp.bfloat16).reshape(sources, 8, width)
            )
            out_ref[here, :, width : width + EXTRA] = extra
            out_ref[here, :, width + EXTRA :] = tail.astype(jnp.bfloat16)

    return kernel


def combine_kernel(micro):
    def kernel(pieces_ref, incoming_ref, inputs_ref, gain_ref, root_ref, pick_a, pick_b, out_ref):
        peers, eight, lanes = pieces_ref.shape
        tokens, width = out_ref.shape
        pieces = pieces_ref[...].reshape(peers * eight, lanes)
        first = dot_first(pick_a[micro], pieces[:, : width + EXTRA])
        second = dot_first(pick_b[micro], pieces[:, width:])
        lane = lax.broadcasted_iota(jnp.int32, (tokens, EXTRA), 1)
        inner = jnp.where(lane < 2, first[:, width:], 0.0) + jnp.where(
            (lane >= 2) & (lane < 4), second[:tokens, :EXTRA], 0.0
        )
        inner = jnp.sum(inner, axis=1, keepdims=True)
        total = first[:, :width] + jnp.concatenate(
            [second[:tokens, EXTRA:], second[tokens:, EXTRA:]], axis=1
        )
        root = root_ref[micro]
        normed = normalized(inputs_ref[micro], root)
        scaled = gain_ref[...] * total
        result = incoming_ref[...].astype(jnp.float32) + (scaled - normed * (inner / D)) / root
        out_ref[...] = result.astype(jnp.bfloat16)

    return kernel


def layers(
    saved_inputs, cot_in, loss_grad, expert_ids, route_weights, norm_gain, w_gate, w_up, w_down
):
    section_count = lax.axis_size("section")
    at_last = lax.axis_index("section") == section_count - 1
    rank = lax.axis_index("tensor").astype(jnp.int32)[None]
    experts = lax.axis_size("expert") // 2
    peers = 2 * experts
    tokens, width = saved_inputs.shape[2:]
    lanes = 3 * width // 2
    hidden = 2 * w_gate.shape[3]
    inputs = saved_inputs[0]
    own = (w_gate[0, 0], w_up[0, 0], w_down[0, 0])

    def like(shape, dtype=jnp.bfloat16):
        return jax.ShapeDtypeStruct(shape, dtype)

    wide = inputs.astype(jnp.float32)
    squares = jnp.sum(wide * wide, axis=2)
    squares = squares + swap(squares)
    root = jnp.sqrt(squares / D + epsilon)[:, :, None]
    slots = peers * 8
    tables = call(
        tables_kernel,
        [
            like((2, slots, tokens)),
            like((2, slots, 2 * tokens)),
            like((2, slots, 1), jnp.float32),
            like((2, slots, 1), jnp.float32),
        ],
        expert_ids[0].transpose(0, 2, 1),
        route_weights[0].transpose(0, 2, 1),
    )
    rows = call(
        pack_kernel, like((peers, 24, lanes)), inputs, cot_in[0], norm_gain, root, *tables
    )
    rows = exchange(rows)
    cross = [diagonal_swap(w) for w in own]
    pair = [pair_swap(w) for w in own]
    far = [pair_swap(w) for w in cross]
    quad = (own, pair, far, cross)
    gates = [w for part in quad for w in part[:2]]
    downs = [part[2] for part in quad]

    def forward(micro):
        return call(
            forward_kernel(16 * micro),
            [like((2 * experts * 8, hidden), jnp.float32)] * 2,
            rows,
            *gates,
            scalar=rank,
        )

    def finish(micro, sums, grads, low, incoming):
        pieces = call(
            backward_kernel(low),
            like((peers, 8, lanes + EXTRA)),
            grads,
            *sums,
            *own,
            scalar=rank,
            outside=(*downs[1:], *gates[2:]),
            scratch=[
                pltpu.VMEM((6, *own[0].shape), jnp.bfloat16),
                pltpu.VMEM((3, *own[2].shape), jnp.bfloat16),
                pltpu.SemaphoreType.DMA((9,)),
            ],
        )
        return call(
            combine_kernel(micro),
            like((tokens, width)),
            exchange(pieces),
            incoming,
            inputs,
            norm_gain,
            root,
            *tables[:2],
        )

    first_grads = finish(0, forward(0), rows, 8, cot_in[0])
    sums_1 = forward(1)
    pairs = [(i, i - 1) for i in range(1, section_count)]
    passed = lax.ppermute(first_grads, "section", pairs)
    incoming = jnp.where(at_last, loss_grad, passed)
    grads_1 = exchange(call(pack_grads_kernel, like((peers, 8, lanes)), incoming, *tables))
    second_grads = finish(1, sums_1, grads_1, 0, incoming)
    return jnp.stack([first_grads, second_grads])[None]


def solution(mesh):
    in_specs = (
        P("section", None, "expert", "tensor"),
        P("section", "expert", "tensor"),
        P("expert", "tensor"),
        P("section", None, "expert", None),
        P("section", None, "expert", None),
        P("section", "tensor"),
        P("section", "expert", "tensor", None),
        P("section", "expert", "tensor", None),
        P("section", "expert", None, "tensor"),
    )
    out_specs = P("section", None, "expert", "tensor")
    return jax.shard_map(layers, mesh=mesh, in_specs=in_specs, out_specs=out_specs, check_vma=False)
```

```python
import jax
import jax.numpy as jnp
from jax import lax
from jax.experimental import pallas as pl
from jax.experimental.pallas import tpu as pltpu
from jax.sharding import PartitionSpec as P

D = 2048
epsilon = 1e-06
LARGE = 24 * 1024 * 1024
SMALL = 12 * 1024 * 1024
EXTRA = 128
SHARE = 12


def call(kernel, out_shape, *operands, scalar=None, outside=(), scratch=()):
    def spec():
        return pl.BlockSpec(memory_space=pltpu.VMEM)

    several = isinstance(out_shape, (list, tuple))
    in_specs = [spec() for _ in operands]
    in_specs += [pl.BlockSpec(memory_space=pltpu.HBM) for _ in outside]
    operands = (*operands, *outside)
    if scalar is not None:
        in_specs = [pl.BlockSpec(memory_space=pltpu.SMEM), *in_specs]
        operands = (scalar, *operands)
    return pl.pallas_call(
        kernel,
        out_shape=out_shape,
        in_specs=in_specs,
        out_specs=[spec() for _ in out_shape] if several else spec(),
        scratch_shapes=scratch,
        compiler_params=pltpu.CompilerParams(
            vmem_limit_bytes=SMALL if scalar is None else LARGE
        ),
    )(*operands)


def dot(left, right):
    return jnp.dot(left, right, preferred_element_type=jnp.float32)


def dot_last(left, right):
    return lax.dot_general(
        left, right, (((1,), (1,)), ((), ())), preferred_element_type=jnp.float32
    )


def dot_first(left, right):
    return lax.dot_general(
        left, right, (((0,), (0,)), ((), ())), preferred_element_type=jnp.float32
    )


def swap(array):
    return lax.ppermute(array, "tensor", [(0, 1), (1, 0)])


def pair_swap(array):
    pairs = [(i, i ^ 1) for i in range(lax.axis_size("expert"))]
    return lax.ppermute(array, "expert", pairs)


def diagonal_swap(array):
    count = lax.axis_size("expert")
    pairs = [(t * count + i, (1 - t) * count + (i ^ 1)) for t in (0, 1) for i in range(count)]
    return lax.ppermute(array, ("tensor", "expert"), pairs)


def exchange(array):
    count = lax.axis_size("expert")
    groups = [
        [t * count + i for t in (0, 1) for i in range(parity, count, 2)] for parity in (0, 1)
    ]
    return lax.all_to_all(
        array,
        ("tensor", "expert"),
        split_axis=0,
        concat_axis=0,
        tiled=True,
        axis_index_groups=groups,
    )


def tables_kernel(ids_ref, weights_ref, pick_a_ref, pick_b_ref, scale_a_ref, scale_b_ref):
    micros, per_token, tokens = ids_ref.shape
    experts = pick_a_ref.shape[1] // 16
    row = lax.broadcasted_iota(jnp.int32, (tokens, tokens), 0)
    col = lax.broadcasted_iota(jnp.int32, (tokens, tokens), 1)
    earlier = (row < col).astype(jnp.bfloat16)
    expert = lax.broadcasted_iota(jnp.int32, (experts, tokens), 0)
    line = lax.broadcasted_iota(jnp.int32, (8, tokens), 0)
    slot_a = line.astype(jnp.float32)
    slot_b = jnp.where(line < 4, line + 8, line + 4).astype(jnp.float32)

    def ones(hit):
        return jnp.where(hit, 1.0, 0.0).astype(jnp.bfloat16)

    for m in range(micros):
        member = jnp.zeros((experts, tokens), jnp.float32)
        weight = jnp.zeros((experts, tokens), jnp.float32)
        for k in range(per_token):
            hit = ids_ref[m, k : k + 1, :] == expert
            member = jnp.where(hit, 1.0, member)
            weight = jnp.where(hit, weights_ref[m, k : k + 1, :], weight)
        before = dot(member.astype(jnp.bfloat16), earlier)
        place = jnp.where(member > 0.0, before, -1.0)
        for rank in range(2):
            for e in range(experts):
                low = (rank * experts + e) * 8
                here = place[e : e + 1, :] - float(rank * SHARE)
                hit_a = slot_a == here
                hit_b = slot_b == here
                pick_a_ref[m, low : low + 8, :] = ones(hit_a)
                pick_b_ref[m, low : low + 8, :tokens] = ones(hit_b & (line < 4))
                pick_b_ref[m, low : low + 8, tokens:] = ones(hit_b & (line >= 4))
                for hit, ref in ((hit_a, scale_a_ref), (hit_b, scale_b_ref)):
                    ref[m, low : low + 8, :] = jnp.sum(
                        jnp.where(hit, weight[e : e + 1, :], 0.0), axis=1, keepdims=True
                    )


def normalized(inputs, root):
    return inputs.astype(jnp.float32) / root


def put(rows, pick_a, pick_b, scales, out_ref, low):
    peers = out_ref.shape[0]
    width = rows.shape[1]
    half = width // 2
    first = dot(pick_a, rows)
    second = dot(pick_b, jnp.concatenate([rows[:, :half], rows[:, half:]], axis=0))
    if scales is not None:
        first = first * scales[0]
        second = second * scales[1]
    out_ref[:, low : low + 8, :width] = first.astype(jnp.bfloat16).reshape(peers, 8, width)
    out_ref[:, low : low + 8, width:] = second.astype(jnp.bfloat16).reshape(peers, 8, half)


def pack_kernel(
    inputs_ref, grads_ref, gain_ref, root_ref, pick_a, pick_b, scale_a, scale_b, out_ref
):
    gain = gain_ref[...]
    for m in (0, 1):
        rows = (normalized(inputs_ref[m], root_ref[m]) * gain).astype(jnp.bfloat16)
        put(rows, pick_a[m], pick_b[m], None, out_ref, 16 * m)
    put(grads_ref[...], pick_a[0], pick_b[0], (scale_a[0], scale_b[0]), out_ref, 8)


def pack_grads_kernel(
    last_ref, loss_ref, passed_ref, pick_a, pick_b, scale_a, scale_b, out_ref, incoming_ref
):
    loss = loss_ref[...].astype(jnp.float32)
    passed = passed_ref[...].astype(jnp.float32)
    incoming = jnp.where(last_ref[0] == 1, loss, passed).astype(jnp.bfloat16)
    incoming_ref[...] = incoming
    put(incoming, pick_a[1], pick_b[1], (scale_a[1], scale_b[1]), out_ref, 0)


def take(ref, start, low, sources):
    part = ref[pl.ds(start, sources), low : low + 8, :]
    width = 2 * part.shape[2] // 3
    tail = part[:, :, width:]
    upper = lax.broadcasted_iota(jnp.int32, tail.shape, 1) < 4
    zero = jnp.zeros_like(tail)
    tail = jnp.concatenate([jnp.where(upper, tail, zero), jnp.where(upper, zero, tail)], axis=2)
    count = sources * 8
    return jnp.concatenate(
        [part[:, :, :width].reshape(count, width), tail.reshape(count, width)], axis=0
    )


def joined(values):
    count = values.shape[0] // 2
    tail = values[count:].reshape(count // 8, 8, values.shape[1])
    tail = tail + pltpu.roll(tail, 4, 1)
    return jnp.concatenate([values[:count], tail.reshape(count, values.shape[1])], axis=0)


def forward_kernel(low):
    def kernel(rank_ref, rows_ref, *refs):
        weights, (gate_ref, up_ref) = refs[:-2], refs[-2:]
        sources = rows_ref.shape[0] // 2
        rank = rank_ref[0]
        parts = [take(rows_ref, place * sources, low, sources) for place in (rank, 1 - rank)]
        half = weights[0].shape[1]
        for kind, out_ref in ((0, gate_ref), (1, up_ref)):
            for f in range(2):
                total = dot(parts[0], weights[2 * f + kind][...])
                total = total + dot(parts[1], weights[4 + 2 * f + kind][...])
                out_ref[:, f * half : (f + 1) * half] = joined(total)

    return kernel


def backward_kernel(low):
    def kernel(rank_ref, grads_ref, gate_ref, up_ref, *refs):
        near, remote, (out_ref, gates_ref, downs_ref, signals) = refs[:3], refs[3:12], refs[12:]
        weights = [near[0], near[1], *(gates_ref.at[i] for i in range(6))]
        downs = [near[2], *(downs_ref.at[i] for i in range(3))]
        copies = [
            pltpu.make_async_copy(source, target, signals.at[i])
            for i, (source, target) in enumerate(zip(remote, [*downs[1:], *weights[2:]]))
        ]
        for copy in copies:
            copy.start()
        peers, _, _ = out_ref.shape
        sources = peers // 2
        count = sources * 8
        half = weights[0].shape[1]
        width = weights[0].shape[0]
        rank = rank_ref[0]
        starts = (rank * sources, (1 - rank) * sources)
        parts = [take(grads_ref, start, low, sources) for start in starts]
        pieces = [0.0, 0.0]
        inner = 0.0
        for copy in copies[:3]:
            copy.wait()
        for f in range(2):
            hidden = dot_last(parts[0], downs[f][...]) + dot_last(parts[1], downs[2 + f][...])
            hidden = joined(hidden)
            gate = gate_ref[:, f * half : (f + 1) * half]
            up = up_ref[:, f * half : (f + 1) * half]
            sigma = jax.nn.sigmoid(gate)
            grad_gate = hidden * up * (sigma * (1.0 + gate * (1.0 - sigma)))
            grad_up = hidden * (gate * sigma)
            inner = inner + jnp.sum(gate * grad_gate + up * grad_up, axis=1, keepdims=True)
            grad_gate = grad_gate.astype(jnp.bfloat16)
            grad_up = grad_up.astype(jnp.bfloat16)
            if f == 0:
                for copy in copies[3:]:
                    copy.wait()
            for i in range(2):
                pieces[i] = pieces[i] + dot_last(grad_gate, weights[4 * i + 2 * f][...])
                pieces[i] = pieces[i] + dot_last(grad_up, weights[4 * i + 2 * f + 1][...])
        coarse = inner.astype(jnp.bfloat16).astype(jnp.float32)
        fine = inner - coarse
        lane = lax.broadcasted_iota(jnp.int32, (count, EXTRA), 1)
        extra = jnp.zeros((count, EXTRA), jnp.float32)
        for place, column in enumerate(
            (coarse[:count], fine[:count], coarse[count:], fine[count:])
        ):
            extra = jnp.where(lane == place, column, extra)
        extra = extra.astype(jnp.bfloat16).reshape(sources, 8, EXTRA)
        upper = lax.broadcasted_iota(jnp.int32, (sources, 8, width // 2), 1) < 4
        for piece, start in zip(pieces, starts):
            tail = piece[count:].reshape(sources, 8, width)
            tail = jnp.where(upper, tail[:, :, : width // 2], tail[:, :, width // 2 :])
            here = pl.ds(start, sources)
            out_ref[here, :, :width] = (
                piece[:count].astype(jnp.bfloat16).reshape(sources, 8, width)
            )
            out_ref[here, :, width : width + EXTRA] = extra
            out_ref[here, :, width + EXTRA :] = tail.astype(jnp.bfloat16)

    return kernel


def combine_kernel(micro):
    def kernel(pieces_ref, incoming_ref, inputs_ref, gain_ref, root_ref, pick_a, pick_b, out_ref):
        peers, eight, lanes = pieces_ref.shape
        tokens, width = out_ref.shape
        pieces = pieces_ref[...].reshape(peers * eight, lanes)
        first = dot_first(pick_a[micro], pieces[:, : width + EXTRA])
        second = dot_first(pick_b[micro], pieces[:, width:])
        lane = lax.broadcasted_iota(jnp.int32, (tokens, EXTRA), 1)
        inner = jnp.where(lane < 2, first[:, width:], 0.0) + jnp.where(
            (lane >= 2) & (lane < 4), second[:tokens, :EXTRA], 0.0
        )
        inner = jnp.sum(inner, axis=1, keepdims=True)
        total = first[:, :width] + jnp.concatenate(
            [second[:tokens, EXTRA:], second[tokens:, EXTRA:]], axis=1
        )
        root = root_ref[micro]
        normed = normalized(inputs_ref[micro], root)
        scaled = gain_ref[...] * total
        result = incoming_ref[...].astype(jnp.float32) + (scaled - normed * (inner / D)) / root
        out_ref[...] = result.astype(jnp.bfloat16)

    return kernel


def layers(
    saved_inputs, cot_in, loss_grad, expert_ids, route_weights, norm_gain, w_gate, w_up, w_down
):
    section_count = lax.axis_size("section")
    at_last = (lax.axis_index("section") == section_count - 1).astype(jnp.int32)[None]
    rank = lax.axis_index("tensor").astype(jnp.int32)[None]
    experts = lax.axis_size("expert") // 2
    peers = 2 * experts
    tokens, width = saved_inputs.shape[2:]
    lanes = 3 * width // 2
    hidden = 2 * w_gate.shape[3]
    inputs = saved_inputs[0]
    own = (w_gate[0, 0], w_up[0, 0], w_down[0, 0])

    def like(shape, dtype=jnp.bfloat16):
        return jax.ShapeDtypeStruct(shape, dtype)

    wide = inputs.astype(jnp.float32)
    squares = jnp.sum(wide * wide, axis=2)
    squares = squares + swap(squares)
    root = jnp.sqrt(squares / D + epsilon)[:, :, None]
    slots = peers * 8
    tables = call(
        tables_kernel,
        [
            like((2, slots, tokens)),
            like((2, slots, 2 * tokens)),
            like((2, slots, 1), jnp.float32),
            like((2, slots, 1), jnp.float32),
        ],
        expert_ids[0].transpose(0, 2, 1),
        route_weights[0].transpose(0, 2, 1),
    )
    rows = call(
        pack_kernel, like((peers, 24, lanes)), inputs, cot_in[0], norm_gain, root, *tables
    )
    rows = exchange(rows)
    cross = [diagonal_swap(w) for w in own]
    pair = [pair_swap(w) for w in own]
    far = [pair_swap(w) for w in cross]
    quad = (own, pair, far, cross)
    gates = [w for part in quad for w in part[:2]]
    downs = [part[2] for part in quad]

    def forward(micro):
        return call(
            forward_kernel(16 * micro),
            [like((2 * experts * 8, hidden), jnp.float32)] * 2,
            rows,
            *gates,
            scalar=rank,
        )

    def finish(micro, sums, grads, low, incoming):
        pieces = call(
            backward_kernel(low),
            like((peers, 8, lanes + EXTRA)),
            grads,
            *sums,
            *own,
            scalar=rank,
            outside=(*downs[1:], *gates[2:]),
            scratch=[
                pltpu.VMEM((6, *own[0].shape), jnp.bfloat16),
                pltpu.VMEM((3, *own[2].shape), jnp.bfloat16),
                pltpu.SemaphoreType.DMA((9,)),
            ],
        )
        return call(
            combine_kernel(micro),
            like((tokens, width)),
            exchange(pieces),
            incoming,
            inputs,
            norm_gain,
            root,
            *tables[:2],
        )

    first_grads = finish(0, forward(0), rows, 8, cot_in[0])
    sums_1 = forward(1)
    pairs = [(i, i - 1) for i in range(1, section_count)]
    passed = lax.ppermute(first_grads, "section", pairs)
    grads_1, incoming = call(
        pack_grads_kernel,
        [like((peers, 8, lanes)), like((tokens, width))],
        loss_grad,
        passed,
        *tables,
        scalar=at_last,
    )
    grads_1 = exchange(grads_1)
    second_grads = finish(1, sums_1, grads_1, 0, incoming)
    return jnp.stack([first_grads, second_grads])[None]


def solution(mesh):
    in_specs = (
        P("section", None, "expert", "tensor"),
        P("section", "expert", "tensor"),
        P("expert", "tensor"),
        P("section", None, "expert", None),
        P("section", None, "expert", None),
        P("section", "tensor"),
        P("section", "expert", "tensor", None),
        P("section", "expert", "tensor", None),
        P("section", "expert", None, "tensor"),
    )
    out_specs = P("section", None, "expert", "tensor")
    return jax.shard_map(layers, mesh=mesh, in_specs=in_specs, out_specs=out_specs, check_vma=False)
```
